512 devices in a mesh: sp: 8 (over z_hi, core), py: 16 (over z_lo, x), pz: 4 (over y).
Axes of the slice: x: 4, y: 4, z: 16 (z_hi: 4, z_lo: 4; z = z_hi * 4 + z_lo), core: 2. Of those that a mesh axis runs over, the one named last changes fastest.
Arguments:
- concentration: float32 [8, 128, 128, 128], P('sp', 'py', 'pz'), may hold values from -1 to 1.1
- mobility: float32 [8, 8], replicated, may hold values from 0.1 to 0.6
- kappa: float32 [8], replicated, may hold values from 0.5 to 2
- well_depth: float32 [8], P('sp'), may hold values from 0.5 to 2
Outputs:
- updated: float32 [8, 128, 128, 128], P('sp', 'py', 'pz')
The draws below stay inside these ranges and needn't reach their ends.
All inputs are finite; a program needn't handle non-finite values.
Results may differ from the reference program's by a relative error of at most 0.000084.
Values sent between devices are 32-bit elements; how exact they have to be, the bound alone decides.
A program may use at most 64 MiB of HBM per device.

```python
import math
import jax
import jax.numpy as jnp
from jax import lax

S = 8
NX = 128
NY = 128
NZ = 128


def draw_concentration(key, part):
    first = jax.random.fold_in(jax.random.fold_in(key, 11), 0)
    base = jax.random.uniform(first, (S, NX, NY, NZ), jnp.float32, -1.0, 1.0)
    return base


def level_of(own_key, extent, cuts, least, top_value):
    factor_of = 1.0
    for position, shards_of in cuts:
        draws = jax.random.uniform(jax.random.fold_in(jax.random.fold_in(own_key, 6), position), (shards_of,), jnp.float32, least / len(cuts), top_value / len(cuts))
        factor_of = factor_of * jnp.repeat(jnp.exp(draws), extent[position] // shards_of).reshape((-1,) + (1,) * (len(extent) - 1 - position))
    return factor_of


def setup_inputs(seed: int = 0) -> dict:
    seeds = jax.random.split(jax.random.key(seed), 5)
    return {
        "concentration": draw_concentration(jax.random.fold_in(seeds[4], 71), 0),
        "mobility": jnp.clip(jax.random.uniform(seeds[1], (S, S), jnp.float32, 0.1, 0.6), 0.1, 0.6),
        "kappa": jnp.clip(jnp.exp(jax.random.uniform(seeds[2], (S,), jnp.float32, math.log(0.5), math.log(2.0))), 0.5, 2.0),
        "well_depth": jnp.clip(jnp.exp(math.log(2.0) - 1.3862944 * jax.random.uniform(seeds[3], (S,), jnp.float32) ** level_of(seeds[3], (S,), ((0, 8),), -0.2, 0.2)), 0.5, 2.0),
    }


def wave_square(count):
    modes = jnp.arange(count, dtype=jnp.int32)
    freq = jnp.where(modes < count // 2, modes, modes - count).astype(jnp.float32)
    return (2.0 * math.pi * freq / count) ** 2


def reference(concentration, mobility, kappa, well_depth):
    conc = concentration
    bulk = well_depth[:, None, None, None] * (conc * conc * conc - conc)
    c_hat = jnp.fft.fftn(conc, axes=(1, 2, 3))
    bulk_hat = jnp.fft.fftn(bulk, axes=(1, 2, 3))
    ksq = wave_square(NX)[:, None, None] + wave_square(NY)[None, :, None] + wave_square(NZ)[None, None, :]
    drive = bulk_hat + kappa[:, None, None, None] * ksq[None] * c_hat
    mix_real = jnp.einsum("ij,jxyz->ixyz", mobility, jnp.real(drive), precision=lax.Precision.HIGHEST)
    mix_imag = jnp.einsum("ij,jxyz->ixyz", mobility, jnp.imag(drive), precision=lax.Precision.HIGHEST)
    mix = mix_real + 1j * mix_imag
    stiff = 0.5 * (jnp.diagonal(mobility) * kappa)[:, None, None, None] * (ksq * ksq)[None]
    new_hat = (c_hat * (1.0 + stiff) - 0.5 * ksq[None] * mix) / (1.0 + stiff)
    updated = jnp.real(jnp.fft.ifftn(new_hat, axes=(1, 2, 3)))
    return updated.astype(jnp.float32)
```

```python
import functools
import math

import jax
import jax.numpy as jnp
import numpy as np
from jax import lax
from jax.experimental import pallas as pl
from jax.experimental.pallas import tpu as pltpu
from jax.sharding import PartitionSpec as P

MESH = pl.DeviceIdType.MESH
N = 128
F32 = jnp.float32
BF16 = jnp.bfloat16


def basis():
    n = np.arange(N)
    out = np.zeros((N, N), np.float64)
    for r in range(N):
        if r == 0:
            out[r] = 1.0 / math.sqrt(N)
        elif r == N // 2:
            out[r] = (1 - 2 * (n % 2)) / math.sqrt(N)
        elif r < N // 2:
            out[r] = np.cos(2 * math.pi * (r * n % N) / N) * math.sqrt(2.0 / N)
        else:
            out[r] = np.sin(2 * math.pi * ((N - r) * n % N) / N) * math.sqrt(2.0 / N)
    return out


def split_table(table):
    table = table.astype(np.float32)
    high = table.astype(BF16)
    low = (table - high.astype(np.float32)).astype(BF16)
    return np.stack([high, low])


def make_tables():
    b = basis()
    y = b.reshape(N, 4, 32)
    fy = np.einsum("kpy,ms->kmpsy", y, np.eye(4)).reshape(512, 512)
    fx = b.reshape(N, 16, 2, 4).transpose(0, 2, 1, 3).reshape(N, N)
    ix = b.T.reshape(16, 2, 4, N).transpose(2, 0, 1, 3).reshape(N, N)
    iy = np.einsum("kpy,ab->paykb", y, np.eye(2)).reshape(256, 256)
    iz = np.broadcast_to(b.reshape(4, 1, 32, N), (4, 4, 32, N)).reshape(512, N)
    return [split_table(t) for t in (b, fy, fx, ix, iy, iz)]


def split(value):
    high = value.astype(BF16)
    return high, (value - high.astype(F32)).astype(BF16)


def dot(a, b, transposed=False):
    dims = (((1,), (1 if transposed else 0,)), ((), ()))
    return lax.dot_general(a, b, dims, preferred_element_type=F32)


def dot3(a, b, transposed=False):
    (ah, al), (bh, bl) = a, b
    return dot(ah, bh, transposed) + (dot(al, bh, transposed) + dot(ah, bl, transposed))


def table(ref):
    return ref[0], ref[1]


def wave(index):
    freq = jnp.where(index < N // 2, index, index - N).astype(F32)
    return (2.0 * math.pi / N * freq) ** 2


def place():
    sp, py = lax.axis_index("sp"), lax.axis_index("py")
    return (sp // 2) * 4 + py // 4, py % 4, sp % 2


def device(z, x, core):
    return {"sp": (z // 4) * 2 + core, "py": (z % 4) * 4 + x}


def offsets():
    order = [8]
    for d in range(7, 0, -1):
        order += [d, 16 - d]
    order += [0]
    return [
        (dz, dx, dc)
        for dz in order
        for dx in (2, 1, 3, 0)
        for dc in (1, 0)
        if (dz, dx, dc) != (0, 0, 0)
    ]


def kernel(
    mob, kap, well, c_hbm, bz_hbm, fy_hbm, fx_hbm, ix_hbm, iy_hbm, iz_hbm, o_ref,
    c, bz, fy, fx, ix, iy, iz, s1, r1, s2, r2, s3, r3, s4, r4, load, send, recv,
):
    z, x, core = place()
    pz = lax.axis_index("pz")
    me = lax.axis_index("sp") * 16 + lax.axis_index("py")
    others = offsets()

    barrier = pltpu.get_barrier_semaphore()
    for k in (1, 2, 3):
        pl.semaphore_signal(barrier, 1, device_id={"pz": (pz + k) % 4}, device_id_type=MESH)
    loads = [
        pltpu.make_async_copy(src, dst, load.at[i])
        for i, (src, dst) in enumerate(
            [(c_hbm, c), (bz_hbm, bz), (fy_hbm, fy), (fx_hbm, fx), (ix_hbm, ix), (iy_hbm, iy), (iz_hbm, iz)]
        )
    ]
    for copy in loads:
        copy.start()

    def peer(offset):
        dz, dx, dc = offset
        return device((z + dz) % 16, (x + dx) % 4, (core + dc) % 2)

    for offset in others:
        pl.semaphore_signal(barrier, 1, device_id=peer(offset), device_id_type=MESH)

    loads[0].wait()
    loads[1].wait()
    conc = c[...].reshape(256, N)
    bulk = well[0] * (conc * conc * conc - conc)
    for f, field in enumerate((conc, bulk)):
        out = dot3(table(bz), split(field), True)
        for p in range(4):
            for h in range(2):
                s1[p, pl.ds(f * 64 + h * 32, 32), :] = out[p * 32 : p * 32 + 32, h * 128 : h * 128 + 128]
    r1[pz] = s1[pz]
    pl.semaphore_wait(barrier, 3 + len(others))
    for k in (2, 1, 3):
        to = (pz + k) % 4
        pltpu.make_async_remote_copy(
            src_ref=s1.at[to], dst_ref=r1.at[pz], send_sem=send.at[0], recv_sem=recv.at[0],
            device_id={"pz": to}, device_id_type=MESH,
        ).start()
    loads[2].wait()
    pltpu.make_async_copy(r1.at[pl.ds(0, 3)], r1.at[pl.ds(0, 3)], recv.at[0]).wait()

    low_high = [split(r1[p]) for p in range(4)]
    high = jnp.concatenate([v[0] for v in low_high], axis=1)
    low = jnp.concatenate([v[1] for v in low_high], axis=1)
    s2[...] = dot3(table(fy), (high, low), True).reshape(N, 4, N)
    r2[me] = s2[me]
    for offset in others:
        to = peer(offset)
        pltpu.make_async_remote_copy(
            src_ref=s2.at[to["sp"] * 16 + to["py"]], dst_ref=r2.at[me], send_sem=send.at[1], recv_sem=recv.at[1],
            device_id=to, device_id_type=MESH,
        ).start()

    lane = lax.broadcasted_iota(jnp.int32, (1, N), 1)
    block = lane // 32

    def lanes(values):
        out = jnp.full((1, N), values[0], F32)
        for q in (1, 2, 3):
            out = jnp.where(block == q, values[q], out)
        return out

    row = lax.broadcasted_iota(jnp.int32, (N, 1), 0)
    ksq = wave(row) + (wave(jnp.full((1, N), me, jnp.int32)) + wave(pz * 32 + lane % 32))
    kappa_ksq = [lanes([kap[4 * h + q] for q in range(4)]) * ksq for h in range(2)]
    factor = []
    for h in range(2):
        stiff = 0.5 * lanes([mob[4 * h + q, 4 * h + q] * kap[4 * h + q] for q in range(4)]) * (ksq * ksq)
        factor.append(0.5 * ksq / (1.0 + stiff))
    coef = [
        [[lanes([mob[4 * hi + q, 4 * hj + (q - s) % 4] for q in range(4)]) for s in range(4)] for hj in range(2)]
        for hi in range(2)
    ]
    loads[3].wait()
    loads[4].wait()
    pltpu.make_async_copy(r2.at[pl.ds(0, 127)], r2.at[pl.ds(0, 127)], recv.at[1]).wait()

    def pick(pieces):
        out = pieces[0]
        for q in (1, 2, 3):
            out = jnp.where(block == q, pieces[q], out)
        return out

    def turn(value, blocks):
        blocks %= 4
        return pltpu.roll(value, blocks * 32, 1) if blocks else value

    hats = [[], []]
    for half in range(2):
        got = [r2[pl.ds((4 * half + q) * 16, 16)].reshape(64, N) for q in range(4)]
        for f in range(2):
            rows = [pick([turn(got[q], q - (2 * f + h)) for q in range(4)]) for h in range(2)]
            hats[f].append(dot3(table(fx), split(jnp.concatenate(rows, axis=0))))
    drive = [hats[1][h] + kappa_ksq[h] * hats[0][h] for h in range(2)]
    turned = [[turn(drive[h], s) for s in range(4)] for h in range(2)]
    for half in range(2):
        mix = sum(coef[half][h][s] * turned[h][s] for h in range(2) for s in range(4))
        new = hats[0][half] - factor[half] * mix
        out = dot3(table(ix), split(new))
        for q in range(4):
            back = pick([turn(out[m * 32 : m * 32 + 32], m - q) for m in range(4)])
            s3[pl.ds((4 * half + q) * 16, 16)] = back.reshape(16, 2, N)
    r3[me] = s3[me]
    for offset in others:
        to = peer(offset)
        pltpu.make_async_remote_copy(
            src_ref=s3.at[to["sp"] * 16 + to["py"]], dst_ref=r3.at[me], send_sem=send.at[2], recv_sem=recv.at[2],
            device_id=to, device_id_type=MESH,
        ).start()
    loads[5].wait()
    loads[6].wait()
    pltpu.make_async_copy(r3.at[pl.ds(0, 127)], r3.at[pl.ds(0, 127)], recv.at[2]).wait()

    s4[...] = dot3(table(iy), split(r3[...].reshape(256, N))).reshape(4, 64, N)
    r4[pz] = s4[pz]
    for k in (2, 1, 3):
        to = (pz + k) % 4
        pltpu.make_async_remote_copy(
            src_ref=s4.at[to], dst_ref=r4.at[pz], send_sem=send.at[3], recv_sem=recv.at[3],
            device_id={"pz": to}, device_id_type=MESH,
        ).start()
    pltpu.make_async_copy(r4.at[pl.ds(0, 3)], r4.at[pl.ds(0, 3)], recv.at[3]).wait()

    lanes4 = jnp.concatenate([r4[p] for p in range(4)], axis=1)
    spot = lax.broadcasted_iota(jnp.int32, (1, 512), 1) // 32 % 4
    masked = jnp.concatenate([jnp.where(spot == m, lanes4, 0.0) for m in range(4)], axis=0)
    out = dot3(split(masked), table(iz))
    for m in range(4):
        for h in range(2):
            o_ref[h * 4 + m] = out[m * 64 + h * 32 : m * 64 + h * 32 + 32, :]

    pltpu.make_async_copy(s1.at[pl.ds(0, 3)], s1.at[pl.ds(0, 3)], send.at[0]).wait()
    pltpu.make_async_copy(s2.at[pl.ds(0, 127)], s2.at[pl.ds(0, 127)], send.at[1]).wait()
    pltpu.make_async_copy(s3.at[pl.ds(0, 127)], s3.at[pl.ds(0, 127)], send.at[2]).wait()
    pltpu.make_async_copy(s4.at[pl.ds(0, 3)], s4.at[pl.ds(0, 3)], send.at[3]).wait()


def per_device(concentration, mobility, kappa, well_depth):
    tables = make_tables()
    smem = pl.BlockSpec(memory_space=pltpu.SMEM)
    hbm = pl.BlockSpec(memory_space=pl.ANY)
    out = pl.pallas_call(
        kernel,
        out_shape=jax.ShapeDtypeStruct((8, 32, N), F32),
        in_specs=[smem] * 3 + [hbm] * 7,
        out_specs=pl.BlockSpec(memory_space=pltpu.VMEM),
        scratch_shapes=[
            pltpu.VMEM((8, 32, N), F32),
            *[pltpu.VMEM(t.shape, BF16) for t in tables],
            pltpu.VMEM((4, N, N), F32),
            pltpu.VMEM((4, N, N), F32),
            pltpu.VMEM((N, 4, N), F32),
            pltpu.VMEM((N, 4, N), F32),
            pltpu.VMEM((N, 2, N), F32),
            pltpu.VMEM((N, 2, N), F32),
            pltpu.VMEM((4, 64, N), F32),
            pltpu.VMEM((4, 64, N), F32),
            pltpu.SemaphoreType.DMA((7,)),
            pltpu.SemaphoreType.DMA((4,)),
            pltpu.SemaphoreType.DMA((4,)),
        ],
        compiler_params=pltpu.CompilerParams(collective_id=0, has_side_effects=True),
    )(mobility, kappa, well_depth, concentration[0], *[jnp.asarray(t) for t in tables])
    return out[None]


def solution(mesh):
    in_specs = (P("sp", "py", "pz", None), P(), P(), P("sp"))
    out_specs = P("sp", "py", "pz", None)
    return jax.shard_map(
        per_device, mesh=mesh, in_specs=in_specs, out_specs=out_specs, check_vma=False
    )
```

```python
import functools
import math

import jax
import jax.numpy as jnp
import numpy as np
from jax import lax
from jax.experimental import pallas as pl
from jax.experimental.pallas import tpu as pltpu
from jax.sharding import PartitionSpec as P

MESH = pl.DeviceIdType.MESH
N = 128
F32 = jnp.float32
BF16 = jnp.bfloat16
LINE = [8, 7, 9, 6, 10, 5, 11, 4, 12, 3, 13, 2, 14, 1, 15]


def basis():
    n = np.arange(N)
    out = np.zeros((N, N), np.float64)
    for r in range(N):
        if r == 0:
            out[r] = 1.0 / math.sqrt(N)
        elif r == N // 2:
            out[r] = (1 - 2 * (n % 2)) / math.sqrt(N)
        elif r < N // 2:
            out[r] = np.cos(2 * math.pi * (r * n % N) / N) * math.sqrt(2.0 / N)
        else:
            out[r] = np.sin(2 * math.pi * ((N - r) * n % N) / N) * math.sqrt(2.0 / N)
    return out


def split_table(table):
    table = table.astype(np.float32)
    high = table.astype(BF16)
    low = (table - high.astype(np.float32)).astype(BF16)
    return np.stack([high, low])


def make_tables():
    b = basis()
    y = b.reshape(N, 4, 32)
    fy = np.einsum("kpy,ed,g->kepgdy", y, np.eye(2), np.ones(2)).reshape(256, 512)
    fx = b.reshape(N, 16, 2, 2, 2).transpose(0, 3, 2, 1, 4).reshape(N, N)
    ix = b.T.reshape(16, 8, N).transpose(1, 0, 2).reshape(N, N)
    iz = b.reshape(4, 2, 16, N).transpose(1, 0, 2, 3).reshape(N, N)
    return [split_table(t) for t in (b, fy, fx, ix, b.T, iz)]


def split(value):
    high = value.astype(BF16)
    return high, (value - high.astype(F32)).astype(BF16)


def dot(a, b, transposed=False):
    dims = (((1,), (1 if transposed else 0,)), ((), ()))
    return lax.dot_general(a, b, dims, preferred_element_type=F32)


def dot3(a, b, transposed=False):
    (ah, al), (bh, bl) = a, b
    return dot(ah, bh, transposed) + (dot(al, bh, transposed) + dot(ah, bl, transposed))


def table(ref):
    return ref[0], ref[1]


def wave(index):
    freq = jnp.where(index < N // 2, index, index - N).astype(F32)
    return (2.0 * math.pi / N * freq) ** 2


def place():
    sp, py = lax.axis_index("sp"), lax.axis_index("py")
    return (sp // 2) * 4 + py // 4, py % 4, sp % 2


def device(z, x, core):
    return {"sp": (z // 4) * 2 + core, "py": (z % 4) * 4 + x}


def offsets():
    return [
        (dz, dx, dc)
        for dz in LINE + [0]
        for dx in (2, 1, 3, 0)
        for dc in (1, 0)
        if (dz, dx, dc) != (0, 0, 0)
    ]


def swap_blocks(values):
    block = lax.broadcasted_iota(jnp.int32, (1, N), 1) // 16
    values = list(values)
    for d in (1, 2, 4):
        low = block // d % 2 == 0
        for i in range(8):
            if i // d % 2 == 0:
                a, b = values[i], values[i + d]
                values[i] = jnp.where(low, a, pltpu.roll(b, 16 * d, 1))
                values[i + d] = jnp.where(low, pltpu.roll(a, N - 16 * d, 1), b)
    return values


def kernel(
    mob, kap, well, c_hbm, bz_hbm, fy_hbm, fx_hbm, ix_hbm, iy_hbm, iz_hbm, o_ref,
    c, bz, fy, fx, ix, iy, iz, s1, r1, s2, r2, s3, r3, s4, r4, load, send, recv, chain,
):
    z, x, core = place()
    pz = lax.axis_index("pz")
    me = lax.axis_index("sp") * 16 + lax.axis_index("py")
    others = offsets()
    barrier = pltpu.get_barrier_semaphore()

    def signal(sem, to):
        pl.semaphore_signal(sem, 1, device_id=to, device_id_type=MESH)

    def peer(offset):
        dz, dx, dc = offset
        return device((z + dz) % 16, (x + dx) % 4, (core + dc) % 2)

    plane = [offset for offset in others if offset[0] == 0]

    for k in (2, 1, 3):
        signal(barrier, {"pz": (pz + k) % 4})
    for dz in LINE:
        signal(barrier, peer((dz, 0, 0)))
    for offset in plane:
        signal(barrier, peer(offset))
    loads = [
        pltpu.make_async_copy(src, dst, load.at[i])
        for i, (src, dst) in enumerate(
            [(c_hbm, c), (bz_hbm, bz), (fy_hbm, fy), (fx_hbm, fx), (ix_hbm, ix), (iy_hbm, iy), (iz_hbm, iz)]
        )
    ]
    for copy in loads:
        copy.start()

    def near(i, src, dst):
        for k in (2, 1, 3):
            to = (pz + k) % 4
            pltpu.make_async_remote_copy(
                src_ref=src.at[to], dst_ref=dst.at[pz], send_sem=send.at[i], recv_sem=recv.at[i],
                device_id={"pz": to}, device_id_type=MESH,
            ).start()

    def far(i, src, dst):
        for offset in others:
            to = peer(offset)
            pltpu.make_async_remote_copy(
                src_ref=src.at[to["sp"] * 16 + to["py"]], dst_ref=dst.at[me],
                send_sem=send.at[i], recv_sem=recv.at[i], device_id=to, device_id_type=MESH,
            ).start()

    def arrive(ref, sem):
        pltpu.make_async_copy(ref, ref, sem).wait()

    loads[0].wait()
    loads[1].wait()
    conc = c[...].reshape(256, N)
    bulk = well[0] * (conc * conc * conc - conc)
    for f, field in enumerate((conc, bulk)):
        out = dot3(table(bz), split(field), True)
        for p in range(4):
            for half in range(2):
                for h in range(2):
                    at = p * 32 + half * 16
                    s1[half, p, pl.ds(f * 32 + h * 16, 16), :] = out[at : at + 16, h * 128 : h * 128 + 128]
    pl.semaphore_wait(barrier, 25)
    for half in range(2):
        near(half, s1.at[half], r1.at[half])
    for offset in plane:
        signal(chain, peer(offset))
    for half in range(2):
        r1[half, pz] = s1[half, pz]
    loads[2].wait()

    left = lax.broadcasted_iota(jnp.int32, (1, N), 1) < 64
    for half in range(2):
        arrive(r1.at[half, pl.ds(0, 3)], recv.at[half])
        parts = []
        for p in range(4):
            value = r1[half, p]
            parts.append(split(jnp.concatenate([jnp.where(left, value, 0.0), jnp.where(left, 0.0, value)], axis=0)))
        both = [jnp.concatenate([v[i] for v in parts], axis=1) for i in range(2)]
        s2[half] = dot3(table(fy), both, True).reshape(N, 2, N)
        if half == 0:
            pl.semaphore_wait(chain, 7)
        far(2 + half, s2.at[half], r2.at[half])
        r2[half, me] = s2[half, me]

    lane = lax.broadcasted_iota(jnp.int32, (1, N), 1)
    block = lane // 16

    def lanes(values):
        out = jnp.full((1, N), values[0], F32)
        for q in range(1, 8):
            out = jnp.where(block == q, values[q], out)
        return out

    row = lax.broadcasted_iota(jnp.int32, (N, 1), 0)
    ksq_xy = wave(row) + wave(jnp.full((1, N), me, jnp.int32))
    kappa = lanes([kap[j] for j in range(8)])
    self_kappa = lanes([mob[j, j] * kap[j] for j in range(8)])
    coef = [lanes([mob[q, (q - s) % 8] for q in range(8)]) for s in range(8)]
    kappa_ksq, factor = [], []
    for half in range(2):
        ksq = ksq_xy + wave(pz * 32 + half * 16 + lane % 16)
        kappa_ksq.append(kappa * ksq)
        factor.append(0.5 * ksq / (1.0 + 0.5 * self_kappa * (ksq * ksq)))
    loads[3].wait()
    loads[4].wait()

    for half in range(2):
        arrive(r2.at[half, pl.ds(0, 127)], recv.at[2 + half])
        got = swap_blocks([r2[half, pl.ds(j * 16, 16)].reshape(32, N) for j in range(8)])
        c_hat, bulk_hat = [
            dot3(table(fx), split(jnp.concatenate([got[g * 4 + f * 2 + h] for g in range(2) for h in range(2)], axis=0)))
            for f in range(2)
        ]
        drive = bulk_hat + kappa_ksq[half] * c_hat
        mix = coef[0] * drive
        for s in range(1, 8):
            mix = mix + coef[s] * pltpu.roll(drive, 16 * s, 1)
        out = dot3(table(ix), split(c_hat - factor[half] * mix))
        back = swap_blocks([out[i * 16 : i * 16 + 16] for i in range(8)])
        for i in range(8):
            s3[half, pl.ds(i * 16, 16)] = back[i].reshape(16, 1, N)
        far(4 + half, s3.at[half], r3.at[half])
        r3[half, me] = s3[half, me]
    loads[5].wait()
    loads[6].wait()

    for half in range(2):
        arrive(r3.at[half, pl.ds(0, 127)], recv.at[4 + half])
        s4[half] = dot3(table(iy), split(r3[half].reshape(N, N))).reshape(4, 32, N)
        near(6 + half, s4.at[half], r4.at[half])
        r4[half, pz] = s4[half, pz]

    for half in range(2):
        arrive(r4.at[half, pl.ds(0, 3)], recv.at[6 + half])
    rows = swap_blocks([r4[half, p] for half in range(2) for p in range(4)])
    out = dot3(split(jnp.concatenate(rows, axis=0)), table(iz))
    o_ref[...] = out.reshape(8, 32, N)

    for half in range(2):
        arrive(s1.at[half, pl.ds(0, 3)], send.at[half])
        arrive(s2.at[half, pl.ds(0, 127)], send.at[2 + half])
        arrive(s3.at[half, pl.ds(0, 127)], send.at[4 + half])
        arrive(s4.at[half, pl.ds(0, 3)], send.at[6 + half])


def per_device(concentration, mobility, kappa, well_depth):
    tables = make_tables()
    smem = pl.BlockSpec(memory_space=pltpu.SMEM)
    hbm = pl.BlockSpec(memory_space=pltpu.HBM)
    in_hbm = [
        pltpu.with_memory_space_constraint(v, pltpu.HBM)
        for v in (mobility, kappa, concentration[0], *map(jnp.asarray, tables))
    ]
    out = pl.pallas_call(
        kernel,
        out_shape=jax.ShapeDtypeStruct((8, 32, N), F32),
        in_specs=[smem] * 3 + [hbm] * 7,
        out_specs=pl.BlockSpec(memory_space=pltpu.VMEM),
        scratch_shapes=[
            pltpu.VMEM((8, 32, N), F32),
            *[pltpu.VMEM(t.shape, BF16) for t in tables],
            pltpu.VMEM((2, 4, 64, N), F32),
            pltpu.VMEM((2, 4, 64, N), F32),
            pltpu.VMEM((2, N, 2, N), F32),
            pltpu.VMEM((2, N, 2, N), F32),
            pltpu.VMEM((2, N, 1, N), F32),
            pltpu.VMEM((2, N, 1, N), F32),
            pltpu.VMEM((2, 4, 32, N), F32),
            pltpu.VMEM((2, 4, 32, N), F32),
            pltpu.SemaphoreType.DMA((7,)),
            pltpu.SemaphoreType.DMA((8,)),
            pltpu.SemaphoreType.DMA((8,)),
            pltpu.SemaphoreType.REGULAR,
        ],
        compiler_params=pltpu.CompilerParams(
            collective_id=0, has_side_effects=True, vmem_limit_bytes=12 * 2**20
        ),
    )(in_hbm[0], in_hbm[1], well_depth, *in_hbm[2:])
    return out[None]


def solution(mesh):
    in_specs = (P("sp", "py", "pz", None), P(), P(), P("sp"))
    out_specs = P("sp", "py", "pz", None)
    return jax.shard_map(
        per_device, mesh=mesh, in_specs=in_specs, out_specs=out_specs, check_vma=False
    )
```

```python
import functools
import math

import jax
import jax.numpy as jnp
import numpy as np
from jax import lax
from jax.experimental import pallas as pl
from jax.experimental.pallas import tpu as pltpu
from jax.sharding import PartitionSpec as P

MESH = pl.DeviceIdType.MESH
N = 128
F32 = jnp.float32
BF16 = jnp.bfloat16
LINE = [8, 7, 9, 6, 10, 5, 11, 4, 12, 3, 13, 2, 14, 1, 15]


def basis():
    n = np.arange(N)
    out = np.zeros((N, N), np.float64)
    for r in range(N):
        if r == 0:
            out[r] = 1.0 / math.sqrt(N)
        elif r == N // 2:
            out[r] = (1 - 2 * (n % 2)) / math.sqrt(N)
        elif r < N // 2:
            out[r] = np.cos(2 * math.pi * (r * n % N) / N) * math.sqrt(2.0 / N)
        else:
            out[r] = np.sin(2 * math.pi * ((N - r) * n % N) / N) * math.sqrt(2.0 / N)
    return out


def split_table(table):
    table = table.astype(np.float32)
    high = table.astype(BF16)
    low = (table - high.astype(np.float32)).astype(BF16)
    return np.stack([high, low])


def make_tables():
    b = basis()
    y = b.reshape(N, 4, 32)
    fy = np.einsum("kpy,ed,g->kepgdy", y, np.eye(2), np.ones(2)).reshape(256, 512)
    fx = b.reshape(N, 16, 2, 2, 2).transpose(0, 3, 2, 1, 4).reshape(N, N)
    ix = b.T.reshape(16, 8, N).transpose(1, 0, 2).reshape(N, N)
    iz = b.reshape(4, 2, 16, N).transpose(1, 0, 2, 3).reshape(N, N)
    return [split_table(t) for t in (b, fy, fx, ix, b.T, iz)]


def split(value):
    high = value.astype(BF16)
    return high, (value - high.astype(F32)).astype(BF16)


def dot(a, b, transposed=False):
    dims = (((1,), (1 if transposed else 0,)), ((), ()))
    return lax.dot_general(a, b, dims, preferred_element_type=F32)


def dot3(a, b, transposed=False):
    (ah, al), (bh, bl) = a, b
    return dot(ah, bh, transposed) + (dot(al, bh, transposed) + dot(ah, bl, transposed))


def table(ref):
    return ref[0], ref[1]


def wave(index):
    freq = jnp.where(index < N // 2, index, index - N).astype(F32)
    return (2.0 * math.pi / N * freq) ** 2


def place():
    sp, py = lax.axis_index("sp"), lax.axis_index("py")
    return (sp // 2) * 4 + py // 4, py % 4, sp % 2


def device(z, x, core):
    return {"sp": (z // 4) * 2 + core, "py": (z % 4) * 4 + x}


def offsets():
    return [
        (dz, dx, dc)
        for dz in LINE + [0]
        for dx in (2, 1, 3, 0)
        for dc in (1, 0)
        if (dz, dx, dc) != (0, 0, 0)
    ]


def swap_blocks(values):
    block = lax.broadcasted_iota(jnp.int32, (1, N), 1) // 16
    values = list(values)
    for d in (1, 2, 4):
        low = block // d % 2 == 0
        for i in range(8):
            if i // d % 2 == 0:
                a, b = values[i], values[i + d]
                values[i] = jnp.where(low, a, pltpu.roll(b, 16 * d, 1))
                values[i + d] = jnp.where(low, pltpu.roll(a, N - 16 * d, 1), b)
    return values


def kernel(
    c_hbm, bz_hbm, fy_hbm, fx_hbm, ix_hbm, iy_hbm, iz_hbm, mob_hbm, kap_hbm, well, o_ref,
    c, bz, fy, fx, ix, iy, iz, mob, kap, s1, r1, s2, r2, s3, r3, s4, r4, load, send, recv, chain,
):
    z, x, core = place()
    pz = lax.axis_index("pz")
    me = lax.axis_index("sp") * 16 + lax.axis_index("py")
    others = offsets()
    barrier = pltpu.get_barrier_semaphore()

    def signal(sem, to):
        pl.semaphore_signal(sem, 1, device_id=to, device_id_type=MESH)

    def peer(offset):
        dz, dx, dc = offset
        return device((z + dz) % 16, (x + dx) % 4, (core + dc) % 2)

    plane = [offset for offset in others if offset[0] == 0]

    for dz in LINE:
        signal(barrier, peer((dz, 0, 0)))
    for k in (2, 1, 3):
        signal(barrier, {"pz": (pz + k) % 4})
    for offset in plane:
        signal(barrier, peer(offset))
    loads = [
        pltpu.make_async_copy(src, dst, load.at[i])
        for i, (src, dst) in enumerate(
            [
                (c_hbm, c), (bz_hbm, bz), (fy_hbm, fy), (fx_hbm, fx), (ix_hbm, ix), (iy_hbm, iy), (iz_hbm, iz),
                (mob_hbm, mob), (kap_hbm, kap),
            ]
        )
    ]
    for copy in loads:
        copy.start()

    def near(i, src, dst):
        for k in (2, 1, 3):
            to = (pz + k) % 4
            pltpu.make_async_remote_copy(
                src_ref=src.at[to], dst_ref=dst.at[pz], send_sem=send.at[i], recv_sem=recv.at[i],
                device_id={"pz": to}, device_id_type=MESH,
            ).start()

    def far(i, src, dst):
        for offset in others:
            to = peer(offset)
            pltpu.make_async_remote_copy(
                src_ref=src.at[to["sp"] * 16 + to["py"]], dst_ref=dst.at[me],
                send_sem=send.at[i], recv_sem=recv.at[i], device_id=to, device_id_type=MESH,
            ).start()

    def arrive(ref, sem):
        pltpu.make_async_copy(ref, ref, sem).wait()

    loads[0].wait()
    loads[1].wait()
    conc = c[...].reshape(256, N)
    bulk = well[0] * (conc * conc * conc - conc)
    for f, field in enumerate((conc, bulk)):
        out = dot3(table(bz), split(field), True)
        for p in range(4):
            for half in range(2):
                for h in range(2):
                    at = p * 32 + half * 16
                    s1[half, p, pl.ds(f * 32 + h * 16, 16), :] = out[at : at + 16, h * 128 : h * 128 + 128]
    pl.semaphore_wait(barrier, 25)
    for half in range(2):
        near(half, s1.at[half], r1.at[half])
    for offset in plane:
        signal(chain, peer(offset))
    for half in range(2):
        r1[half, pz] = s1[half, pz]
    loads[2].wait()

    left = lax.broadcasted_iota(jnp.int32, (1, N), 1) < 64
    for half in range(2):
        arrive(r1.at[half, pl.ds(0, 3)], recv.at[half])
        parts = []
        for p in range(4):
            value = r1[half, p]
            parts.append(split(jnp.concatenate([jnp.where(left, value, 0.0), jnp.where(left, 0.0, value)], axis=0)))
        both = [jnp.concatenate([v[i] for v in parts], axis=1) for i in range(2)]
        s2[half] = dot3(table(fy), both, True).reshape(N, 2, N)
        if half == 0:
            pl.semaphore_wait(chain, 7)
        far(2 + half, s2.at[half], r2.at[half])
        r2[half, me] = s2[half, me]

    lane = lax.broadcasted_iota(jnp.int32, (1, N), 1)
    block = lane // 16

    def lanes(values):
        out = jnp.full((1, N), values[0], F32)
        for q in range(1, 8):
            out = jnp.where(block == q, values[q], out)
        return out

    loads[7].wait()
    loads[8].wait()
    row = lax.broadcasted_iota(jnp.int32, (N, 1), 0)
    ksq_xy = wave(row) + wave(jnp.full((1, N), me, jnp.int32))
    kappa = lanes([kap[j] for j in range(8)])
    self_kappa = lanes([mob[j, j] * kap[j] for j in range(8)])
    coef = [lanes([mob[q, (q - s) % 8] for q in range(8)]) for s in range(8)]
    kappa_ksq, factor = [], []
    for half in range(2):
        ksq = ksq_xy + wave(pz * 32 + half * 16 + lane % 16)
        kappa_ksq.append(kappa * ksq)
        factor.append(0.5 * ksq / (1.0 + 0.5 * self_kappa * (ksq * ksq)))
    loads[3].wait()
    loads[4].wait()

    for half in range(2):
        arrive(r2.at[half, pl.ds(0, 127)], recv.at[2 + half])
        got = swap_blocks([r2[half, pl.ds(j * 16, 16)].reshape(32, N) for j in range(8)])
        c_hat, bulk_hat = [
            dot3(table(fx), split(jnp.concatenate([got[g * 4 + f * 2 + h] for g in range(2) for h in range(2)], axis=0)))
            for f in range(2)
        ]
        drive = bulk_hat + kappa_ksq[half] * c_hat
        mix = coef[0] * drive
        for s in range(1, 8):
            mix = mix + coef[s] * pltpu.roll(drive, 16 * s, 1)
        out = dot3(table(ix), split(c_hat - factor[half] * mix))
        back = swap_blocks([out[i * 16 : i * 16 + 16] for i in range(8)])
        for i in range(8):
            s3[half, pl.ds(i * 16, 16)] = back[i].reshape(16, 1, N)
        far(4 + half, s3.at[half], r3.at[half])
        r3[half, me] = s3[half, me]
    loads[5].wait()
    loads[6].wait()

    for half in range(2):
        arrive(r3.at[half, pl.ds(0, 127)], recv.at[4 + half])
        s4[half] = dot3(table(iy), split(r3[half].reshape(N, N))).reshape(4, 32, N)
        near(6 + half, s4.at[half], r4.at[half])
        r4[half, pz] = s4[half, pz]

    for half in range(2):
        arrive(r4.at[half, pl.ds(0, 3)], recv.at[6 + half])
    rows = swap_blocks([r4[half, p] for half in range(2) for p in range(4)])
    out = dot3(split(jnp.concatenate(rows, axis=0)), table(iz))
    o_ref[...] = out.reshape(8, 32, N)

    for half in range(2):
        arrive(s1.at[half, pl.ds(0, 3)], send.at[half])
        arrive(s2.at[half, pl.ds(0, 127)], send.at[2 + half])
        arrive(s3.at[half, pl.ds(0, 127)], send.at[4 + half])
        arrive(s4.at[half, pl.ds(0, 3)], send.at[6 + half])


def per_device(concentration, mobility, kappa, well_depth):
    tables = make_tables()
    hbm = pl.BlockSpec(memory_space=pltpu.HBM)
    in_hbm = [
        pltpu.with_memory_space_constraint(v, pltpu.HBM)
        for v in (concentration[0], *map(jnp.asarray, tables), mobility, kappa)
    ]
    out = pl.pallas_call(
        kernel,
        out_shape=jax.ShapeDtypeStruct((8, 32, N), F32),
        in_specs=[hbm] * 9 + [pl.BlockSpec(memory_space=pltpu.SMEM)],
        out_specs=pl.BlockSpec(memory_space=pltpu.VMEM),
        scratch_shapes=[
            pltpu.VMEM((8, 32, N), F32),
            *[pltpu.VMEM(t.shape, BF16) for t in tables],
            pltpu.SMEM((8, 8), F32),
            pltpu.SMEM((8,), F32),
            pltpu.VMEM((2, 4, 64, N), F32),
            pltpu.VMEM((2, 4, 64, N), F32),
            pltpu.VMEM((2, N, 2, N), F32),
            pltpu.VMEM((2, N, 2, N), F32),
            pltpu.VMEM((2, N, 1, N), F32),
            pltpu.VMEM((2, N, 1, N), F32),
            pltpu.VMEM((2, 4, 32, N), F32),
            pltpu.VMEM((2, 4, 32, N), F32),
            pltpu.SemaphoreType.DMA((10,)),
            pltpu.SemaphoreType.DMA((8,)),
            pltpu.SemaphoreType.DMA((8,)),
            pltpu.SemaphoreType.REGULAR,
        ],
        compiler_params=pltpu.CompilerParams(
            collective_id=0, has_side_effects=True, vmem_limit_bytes=12 * 2**20
        ),
    )(*in_hbm, well_depth)
    return out[None]


def solution(mesh):
    in_specs = (P("sp", "py", "pz", None), P(), P(), P("sp"))
    out_specs = P("sp", "py", "pz", None)
    return jax.shard_map(
        per_device, mesh=mesh, in_specs=in_specs, out_specs=out_specs, check_vma=False
    )
```

```python
import functools
import math

import jax
import jax.numpy as jnp
import numpy as np
from jax import lax
from jax.experimental import pallas as pl
from jax.experimental.pallas import tpu as pltpu
from jax.sharding import PartitionSpec as P

MESH = pl.DeviceIdType.MESH
N = 128
F32 = jnp.float32
BF16 = jnp.bfloat16
LINE = [8, 7, 9, 6, 10, 5, 11, 4, 12, 3, 13, 2, 14, 1, 15]


def basis():
    n = np.arange(N)
    out = np.zeros((N, N), np.float64)
    for r in range(N):
        if r == 0:
            out[r] = 1.0 / math.sqrt(N)
        elif r == N // 2:
            out[r] = (1 - 2 * (n % 2)) / math.sqrt(N)
        elif r < N // 2:
            out[r] = np.cos(2 * math.pi * (r * n % N) / N) * math.sqrt(2.0 / N)
        else:
            out[r] = np.sin(2 * math.pi * ((N - r) * n % N) / N) * math.sqrt(2.0 / N)
    return out


def split_table(table):
    table = table.astype(np.float32)
    high = table.astype(BF16)
    low = (table - high.astype(np.float32)).astype(BF16)
    return np.stack([high, low])


def make_tables():
    b = basis()
    y = b.reshape(N, 4, 32)
    fy = np.einsum("kpy,ed,g->kepgdy", y, np.eye(2), np.ones(2)).reshape(256, 512)
    fx = b.reshape(N, 16, 2, 2, 2).transpose(0, 3, 2, 1, 4).reshape(N, N)
    ix = b.T.reshape(16, 8, N).transpose(1, 0, 2).reshape(N, N)
    iz = b.reshape(4, 2, 16, N).transpose(1, 0, 2, 3).reshape(N, N)
    return [split_table(t) for t in (b, fy, fx, ix, b.T, iz)]


def split(value):
    high = value.astype(BF16)
    return high, (value - high.astype(F32)).astype(BF16)


def dot(a, b, transposed=False):
    dims = (((1,), (1 if transposed else 0,)), ((), ()))
    return lax.dot_general(a, b, dims, preferred_element_type=F32)


def dot3(a, b, transposed=False):
    (ah, al), (bh, bl) = a, b
    return dot(ah, bh, transposed) + (dot(al, bh, transposed) + dot(ah, bl, transposed))


def table(ref):
    return ref[0], ref[1]


def wave(index):
    freq = jnp.where(index < N // 2, index, index - N).astype(F32)
    return (2.0 * math.pi / N * freq) ** 2


def place():
    sp, py = lax.axis_index("sp"), lax.axis_index("py")
    return (sp // 2) * 4 + py // 4, py % 4, sp % 2


def device(z, x, core):
    return {"sp": (z // 4) * 2 + core, "py": (z % 4) * 4 + x}


def offsets():
    return [
        (dz, dx, dc)
        for dz in LINE + [0]
        for dx in (2, 1, 3, 0)
        for dc in (1, 0)
        if (dz, dx, dc) != (0, 0, 0)
    ]


def swap_blocks(values):
    block = lax.broadcasted_iota(jnp.int32, (1, N), 1) // 16
    values = list(values)
    for d in (1, 2, 4):
        low = block // d % 2 == 0
        for i in range(8):
            if i // d % 2 == 0:
                a, b = values[i], values[i + d]
                values[i] = jnp.where(low, a, pltpu.roll(b, 16 * d, 1))
                values[i + d] = jnp.where(low, pltpu.roll(a, N - 16 * d, 1), b)
    return values


def kernel(
    c_hbm, bz_hbm, fy_hbm, fx_hbm, ix_hbm, iy_hbm, iz_hbm, mob_hbm, kap_hbm, well, o_ref,
    c, bz, fy, fx, ix, iy, iz, mob, kap, s1, r1, s2, r2, s3, r3, s4, r4, load, send, recv, chain, ready,
):
    z, x, core = place()
    pz = lax.axis_index("pz")
    me = lax.axis_index("sp") * 16 + lax.axis_index("py")
    others = offsets()
    barrier = pltpu.get_barrier_semaphore()

    def signal(sem, to):
        pl.semaphore_signal(sem, 1, device_id=to, device_id_type=MESH)

    def peer(offset):
        dz, dx, dc = offset
        return device((z + dz) % 16, (x + dx) % 4, (core + dc) % 2)

    plane = [offset for offset in others if offset[0] == 0]

    loads = [
        pltpu.make_async_copy(src, dst, load.at[i])
        for i, (src, dst) in enumerate(
            [
                (c_hbm, c), (bz_hbm, bz), (fy_hbm, fy), (fx_hbm, fx), (ix_hbm, ix), (iy_hbm, iy), (iz_hbm, iz),
                (mob_hbm, mob), (kap_hbm, kap),
            ]
        )
    ]
    for copy in loads:
        copy.start()

    for dz in LINE:
        signal(barrier, device((z + dz) % 16, x, 0))
    for k in (2, 1, 3):
        signal(barrier, {"pz": (pz + k) % 4, **device(z, x, 1)})
    signal(barrier, device(z, x, 1 - core))
    for dx in (2, 1, 3):
        signal(barrier, device(z, (x + dx) % 4, 0))
    def near(i, src, dst):
        for k in (2, 1, 3):
            to = (pz + k) % 4
            pltpu.make_async_remote_copy(
                src_ref=src.at[to], dst_ref=dst.at[pz], send_sem=send.at[i], recv_sem=recv.at[i],
                device_id={"pz": to}, device_id_type=MESH,
            ).start()

    def far(i, src, dst):
        for offset in others:
            to = peer(offset)
            pltpu.make_async_remote_copy(
                src_ref=src.at[to["sp"] * 16 + to["py"]], dst_ref=dst.at[me],
                send_sem=send.at[i], recv_sem=recv.at[i], device_id=to, device_id_type=MESH,
            ).start()

    def arrive(ref, sem):
        pltpu.make_async_copy(ref, ref, sem).wait()

    loads[0].wait()
    loads[1].wait()
    conc = c[...].reshape(256, N)
    bulk = well[0] * (conc * conc * conc - conc)
    for f, field in enumerate((conc, bulk)):
        out = dot3(table(bz), split(field), True)
        for p in range(4):
            for half in range(2):
                for h in range(2):
                    at = p * 32 + half * 16
                    s1[half, p, pl.ds(f * 32 + h * 16, 16), :] = out[at : at + 16, h * 128 : h * 128 + 128]
    @pl.when(core == 1)
    def _():
        pl.semaphore_wait(barrier, 7)
        signal(ready, device(z, x, 0))

    @pl.when(core == 0)
    def _():
        pl.semaphore_wait(ready, 1)

    for half in range(2):
        near(half, s1.at[half], r1.at[half])
    for half in range(2):
        r1[half, pz] = s1[half, pz]

    @pl.when(core == 0)
    def _():
        pl.semaphore_wait(barrier, 37)
        for offset in plane:
            signal(chain, peer(offset))

    loads[2].wait()

    left = lax.broadcasted_iota(jnp.int32, (1, N), 1) < 64
    for half in range(2):
        arrive(r1.at[half, pl.ds(0, 3)], recv.at[half])
        parts = []
        for p in range(4):
            value = r1[half, p]
            parts.append(split(jnp.concatenate([jnp.where(left, value, 0.0), jnp.where(left, 0.0, value)], axis=0)))
        both = [jnp.concatenate([v[i] for v in parts], axis=1) for i in range(2)]
        s2[half] = dot3(table(fy), both, True).reshape(N, 2, N)
        if half == 0:
            pl.semaphore_wait(chain, jnp.where(core == 0, 3, 4))
        far(2 + half, s2.at[half], r2.at[half])
        r2[half, me] = s2[half, me]

    lane = lax.broadcasted_iota(jnp.int32, (1, N), 1)
    block = lane // 16

    def lanes(values):
        out = jnp.full((1, N), values[0], F32)
        for q in range(1, 8):
            out = jnp.where(block == q, values[q], out)
        return out

    loads[7].wait()
    loads[8].wait()
    row = lax.broadcasted_iota(jnp.int32, (N, 1), 0)
    ksq_xy = wave(row) + wave(jnp.full((1, N), me, jnp.int32))
    kappa = lanes([kap[j] for j in range(8)])
    self_kappa = lanes([mob[j, j] * kap[j] for j in range(8)])
    coef = [lanes([mob[q, (q - s) % 8] for q in range(8)]) for s in range(8)]
    kappa_ksq, factor = [], []
    for half in range(2):
        ksq = ksq_xy + wave(pz * 32 + half * 16 + lane % 16)
        kappa_ksq.append(kappa * ksq)
        factor.append(0.5 * ksq / (1.0 + 0.5 * self_kappa * (ksq * ksq)))
    loads[3].wait()
    loads[4].wait()

    for half in range(2):
        arrive(r2.at[half, pl.ds(0, 127)], recv.at[2 + half])
        got = swap_blocks([r2[half, pl.ds(j * 16, 16)].reshape(32, N) for j in range(8)])
        c_hat, bulk_hat = [
            dot3(table(fx), split(jnp.concatenate([got[g * 4 + f * 2 + h] for g in range(2) for h in range(2)], axis=0)))
            for f in range(2)
        ]
        drive = bulk_hat + kappa_ksq[half] * c_hat
        mix = coef[0] * drive
        for s in range(1, 8):
            mix = mix + coef[s] * pltpu.roll(drive, 16 * s, 1)
        out = dot3(table(ix), split(c_hat - factor[half] * mix))
        back = swap_blocks([out[i * 16 : i * 16 + 16] for i in range(8)])
        for i in range(8):
            s3[half, pl.ds(i * 16, 16)] = back[i].reshape(16, 1, N)
        far(4 + half, s3.at[half], r3.at[half])
        r3[half, me] = s3[half, me]
    loads[5].wait()
    loads[6].wait()

    for half in range(2):
        arrive(r3.at[half, pl.ds(0, 127)], recv.at[4 + half])
        s4[half] = dot3(table(iy), split(r3[half].reshape(N, N))).reshape(4, 32, N)
        near(6 + half, s4.at[half], r4.at[half])
        r4[half, pz] = s4[half, pz]

    for half in range(2):
        arrive(r4.at[half, pl.ds(0, 3)], recv.at[6 + half])
    rows = swap_blocks([r4[half, p] for half in range(2) for p in range(4)])
    out = dot3(split(jnp.concatenate(rows, axis=0)), table(iz))
    o_ref[...] = out.reshape(8, 32, N)

    for half in range(2):
        arrive(s1.at[half, pl.ds(0, 3)], send.at[half])
        arrive(s2.at[half, pl.ds(0, 127)], send.at[2 + half])
        arrive(s3.at[half, pl.ds(0, 127)], send.at[4 + half])
        arrive(s4.at[half, pl.ds(0, 3)], send.at[6 + half])


def per_device(concentration, mobility, kappa, well_depth):
    tables = make_tables()
    hbm = pl.BlockSpec(memory_space=pltpu.HBM)
    in_hbm = [
        pltpu.with_memory_space_constraint(v, pltpu.HBM)
        for v in (concentration[0], *map(jnp.asarray, tables), mobility, kappa)
    ]
    out = pl.pallas_call(
        kernel,
        out_shape=jax.ShapeDtypeStruct((8, 32, N), F32),
        in_specs=[hbm] * 9 + [pl.BlockSpec(memory_space=pltpu.SMEM)],
        out_specs=pl.BlockSpec(memory_space=pltpu.VMEM),
        scratch_shapes=[
            pltpu.VMEM((8, 32, N), F32),
            *[pltpu.VMEM(t.shape, BF16) for t in tables],
            pltpu.SMEM((8, 8), F32),
            pltpu.SMEM((8,), F32),
            pltpu.VMEM((2, 4, 64, N), F32),
            pltpu.VMEM((2, 4, 64, N), F32),
            pltpu.VMEM((2, N, 2, N), F32),
            pltpu.VMEM((2, N, 2, N), F32),
            pltpu.VMEM((2, N, 1, N), F32),
            pltpu.VMEM((2, N, 1, N), F32),
            pltpu.VMEM((2, 4, 32, N), F32),
            pltpu.VMEM((2, 4, 32, N), F32),
            pltpu.SemaphoreType.DMA((10,)),
            pltpu.SemaphoreType.DMA((8,)),
            pltpu.SemaphoreType.DMA((8,)),
            pltpu.SemaphoreType.REGULAR,
            pltpu.SemaphoreType.REGULAR,
        ],
        compiler_params=pltpu.CompilerParams(
            collective_id=0, has_side_effects=True, vmem_limit_bytes=12 * 2**20
        ),
    )(*in_hbm, well_depth)
    return out[None]


def solution(mesh):
    in_specs = (P("sp", "py", "pz", None), P(), P(), P("sp"))
    out_specs = P("sp", "py", "pz", None)
    return jax.shard_map(
        per_device, mesh=mesh, in_specs=in_specs, out_specs=out_specs, check_vma=False
    )
```
